8 devices in a mesh: dp: 1 (over z), ep: 8 (over y, x, core).
Axes of the slice: x: 2, y: 2, z: 1, core: 2. Of those that a mesh axis runs over, the one named last changes fastest.
Arguments:
- x_in: bfloat16 [128, 512, 768], P(('dp', 'ep'))
- pad_mask: int32 [128, 512], P(('dp', 'ep'))
- rel_bias: float32 [12, 512, 512], replicated
- expert_idx: int32 [2, 128, 512], P(None, ('dp', 'ep'))
- norm_scale: float32 [2, 2, 768], replicated
- w_query: bfloat16 [2, 768, 768], replicated
- w_key: bfloat16 [2, 768, 768], replicated
- w_value: bfloat16 [2, 768, 768], replicated
- w_attn_out: bfloat16 [2, 768, 768], replicated
- w_router: float32 [2, 768, 16], replicated
- w_in: bfloat16 [2, 16, 768, 3072], P(None, 'ep')
- w_out: bfloat16 [2, 16, 3072, 768], P(None, 'ep')
Outputs:
- output: bfloat16 [128, 512, 768], P(('dp', 'ep'))
All inputs are finite; a program needn't handle non-finite values.
Results may differ from the reference program's by a relative error of at most 0.0190526.
Values are sent between devices in bfloat16 or wider.
A program may use at most 1 GiB of HBM per device.

```python
import jax
import jax.numpy as jnp
from jax import lax

SEQS = 16
SEQ = 512
D = 768
HEADS = 12
HEAD = 64
FF = 3072
EXPERTS = 16
GROUPS = 8
CAP_FACTOR = 2
NORM_EPS = 1e-6
NEG_BIG = -1e9
TOKENS = SEQS * SEQ
NUM_SEQ = GROUPS * SEQS
INNER = HEADS * HEAD
CAPACITY = (CAP_FACTOR * TOKENS + EXPERTS - 1) // EXPERTS


def draw_mask(rng_key, num_seq):
    lengths = jax.random.randint(rng_key, (num_seq,), SEQ // 4, SEQ + 1)
    return (jnp.arange(SEQ)[None, :] < lengths[:, None]).astype(jnp.int32)


def draw_routes(rng_key, num_seq):
    route_keys = jax.random.split(rng_key, 5)
    rank_draws = [jax.random.randint(route_keys[draw_id], (2, num_seq, SEQ), 0, EXPERTS) for draw_id in range(3)]
    ranks = jnp.minimum(jnp.minimum(rank_draws[0], rank_draws[1]), rank_draws[2])
    perm_first = jax.random.permutation(route_keys[3], EXPERTS)
    perm_second = jax.random.permutation(route_keys[4], EXPERTS)
    return jnp.stack([perm_first[ranks[0]], perm_second[ranks[1]]]).astype(jnp.int32)


def setup_inputs(seed: int = 0, part: int = 0) -> dict:
    base_key = jax.random.key(seed)
    part_keys = jax.random.split(jax.random.fold_in(base_key, part), 3)
    shared_keys = jax.random.split(base_key, 10)
    x_in = jax.random.normal(part_keys[0], (NUM_SEQ, SEQ, D), jnp.float32).astype(jnp.bfloat16)
    pad_mask = draw_mask(part_keys[1], NUM_SEQ)
    expert_idx = draw_routes(part_keys[2], NUM_SEQ)
    rel_bias = 2.0 * jax.random.normal(shared_keys[0], (HEADS, SEQ, SEQ), jnp.float32)
    norm_scale = jax.random.uniform(shared_keys[1], (2, 2, D), jnp.float32, 0.5, 1.5)
    qk_std = (2.0 / D) ** 0.5 * HEAD ** -0.25
    w_query = (qk_std * jax.random.normal(shared_keys[2], (2, D, INNER), jnp.float32)).astype(jnp.bfloat16)
    w_key = (qk_std * jax.random.normal(shared_keys[3], (2, D, INNER), jnp.float32)).astype(jnp.bfloat16)
    w_value = (D ** -0.5 * jax.random.normal(shared_keys[4], (2, D, INNER), jnp.float32)).astype(jnp.bfloat16)
    w_attn_out = (INNER ** -0.5 * jax.random.normal(shared_keys[5], (2, INNER, D), jnp.float32)).astype(jnp.bfloat16)
    w_router = D ** -0.5 * jax.random.normal(shared_keys[6], (2, D, EXPERTS), jnp.float32)
    w_in = (D ** -0.5 * jax.random.normal(shared_keys[7], (2, EXPERTS, D, FF), jnp.float32)).astype(jnp.bfloat16)
    w_out = (EXPERTS * FF ** -0.5 * jax.random.normal(shared_keys[8], (2, EXPERTS, FF, D), jnp.float32)).astype(jnp.bfloat16)
    return dict(x_in=x_in, pad_mask=pad_mask, rel_bias=rel_bias, expert_idx=expert_idx, norm_scale=norm_scale, w_query=w_query, w_key=w_key, w_value=w_value, w_attn_out=w_attn_out, w_router=w_router, w_in=w_in, w_out=w_out)


def rms_norm(hidden, gain):
    hid32 = hidden.astype(jnp.float32)
    return hid32 * lax.rsqrt(jnp.mean(hid32 * hid32, axis=-1, keepdims=True) + NORM_EPS) * gain


def attention_block(hidden, pad_mask, rel_bias, gain, query_w, key_w, value_w, out_w):
    def one_sequence(seq_pair):
        seq_rows, seq_mask = seq_pair
        normed = rms_norm(seq_rows, gain).astype(jnp.bfloat16)
        query_rows = jnp.dot(normed, query_w, preferred_element_type=jnp.float32).astype(jnp.bfloat16).reshape(SEQ, HEADS, HEAD)
        key_rows = jnp.dot(normed, key_w, preferred_element_type=jnp.float32).astype(jnp.bfloat16).reshape(SEQ, HEADS, HEAD)
        value_rows = jnp.dot(normed, value_w, preferred_element_type=jnp.float32).astype(jnp.bfloat16).reshape(SEQ, HEADS, HEAD)
        scores = jnp.einsum('qhd,khd->hqk', query_rows.astype(jnp.float32), key_rows.astype(jnp.float32))
        scores = scores + rel_bias + jnp.where(seq_mask > 0, 0.0, NEG_BIG)[None, None, :]
        attn_probs = jax.nn.softmax(scores, axis=-1).astype(jnp.bfloat16)
        context = jnp.einsum('hqk,khd->qhd', attn_probs.astype(jnp.float32), value_rows.astype(jnp.float32))
        context = context.astype(jnp.bfloat16).reshape(SEQ, INNER)
        attn_out = jnp.dot(context, out_w, preferred_element_type=jnp.float32)
        return (seq_rows.astype(jnp.float32) + attn_out).astype(jnp.bfloat16)
    return lax.map(one_sequence, (hidden, pad_mask))


def expert_block(hidden, layer_ids, gain, route_w, up_w, down_w):
    grouped = hidden.reshape(GROUPS, TOKENS, D)
    ids_grouped = layer_ids.reshape(GROUPS, TOKENS)

    def route_group(grp_pair):
        grp_rows, grp_ids = grp_pair
        normed32 = rms_norm(grp_rows, gain)
        logits = jnp.dot(normed32, route_w, preferred_element_type=jnp.float32)
        gate_val = jnp.take_along_axis(jax.nn.softmax(logits, axis=-1), grp_ids[:, None], axis=1)[:, 0]
        one_hot = (grp_ids[:, None] == jnp.arange(EXPERTS)[None, :]).astype(jnp.int32)
        token_slot = jnp.take_along_axis(jnp.cumsum(one_hot, axis=0), grp_ids[:, None], axis=1)[:, 0] - 1
        flat_slot = jnp.where(token_slot < CAPACITY, grp_ids * CAPACITY + token_slot, EXPERTS * CAPACITY)
        slot_token = jnp.full((EXPERTS * CAPACITY,), TOKENS, jnp.int32).at[flat_slot].set(jnp.arange(TOKENS, dtype=jnp.int32), mode='drop')
        packed = jnp.take(normed32.astype(jnp.bfloat16), slot_token, axis=0, mode='fill', fill_value=0)
        return packed.reshape(EXPERTS, CAPACITY, D), gate_val, flat_slot

    packed, gate_val, flat_slot = lax.map(route_group, (grouped, ids_grouped))

    def one_expert(expert_parts):
        exp_rows, exp_up, exp_down = expert_parts
        flat_rows = exp_rows.reshape(GROUPS * CAPACITY, D)
        inner_act = jnp.maximum(jnp.dot(flat_rows, exp_up, preferred_element_type=jnp.float32), 0.0).astype(jnp.bfloat16)
        return jnp.dot(inner_act, exp_down, preferred_element_type=jnp.float32).astype(jnp.bfloat16).reshape(GROUPS, CAPACITY, D)

    expert_rows = lax.map(one_expert, (jnp.swapaxes(packed, 0, 1), up_w, down_w))
    expert_rows = jnp.swapaxes(expert_rows, 0, 1).reshape(GROUPS, EXPERTS * CAPACITY, D)

    def combine(grp_parts):
        grp_rows, grp_out, grp_gate, grp_flat = grp_parts
        returned = jnp.take(grp_out, grp_flat, axis=0, mode='fill', fill_value=0)
        return (grp_rows.astype(jnp.float32) + grp_gate[:, None] * returned.astype(jnp.float32)).astype(jnp.bfloat16)

    return lax.map(combine, (grouped, expert_rows, gate_val, flat_slot)).reshape(NUM_SEQ, SEQ, D)


def reference(x_in, pad_mask, rel_bias, expert_idx, norm_scale, w_query, w_key, w_value, w_attn_out, w_router, w_in, w_out):
    def layer_step(hidden, layer_params):
        gains, query_w, key_w, value_w, out_w, route_w, up_w, down_w, layer_ids = layer_params
        hidden = attention_block(hidden, pad_mask, rel_bias, gains[0], query_w, key_w, value_w, out_w)
        hidden = expert_block(hidden, layer_ids, gains[1], route_w, up_w, down_w)
        return hidden, None
    final_state = lax.scan(layer_step, x_in, (norm_scale, w_query, w_key, w_value, w_attn_out, w_router, w_in, w_out, expert_idx))
    return final_state[0]
```

```python
import functools

import jax
import jax.numpy as jnp
import numpy as np
from jax import lax
from jax.experimental import pallas as pl
from jax.experimental.pallas import tpu as pltpu
from jax.sharding import PartitionSpec as P

NORM_EPS = 1e-6
NEG_BIG = -1e9
CAP_FACTOR = 2
BF = jnp.bfloat16
F32 = jnp.float32
I32 = jnp.int32

BLK = 16
LOCAL = 64
TILE = 16
PER_CHIP = 4
LANES = 128
CHUNKS = (6, 10)
VMEM = 60 << 20


def dot(a, b):
    return jnp.dot(a, b, preferred_element_type=F32)


def dot_nt(a, b):
    return lax.dot_general(a, b, (((1,), (1,)), ((), ())), preferred_element_type=F32)


def rms(h32, gain):
    return h32 * lax.rsqrt(jnp.mean(h32 * h32, axis=-1, keepdims=True) + NORM_EPS) * gain


def route_kernel(idx_ref, low_ref, up_ref, comb_ref, tbl_ref, cnt_ref, *, cap, experts):
    layers, rows, _ = idx_ref.shape
    seqs = comb_ref.shape[1]
    per_seq = rows // seqs
    lane = lax.broadcasted_iota(I32, (rows, LANES), 1)
    for l in range(layers):
        x = idx_ref[l]
        hits = [x == e for e in range(experts)]
        stack = jnp.concatenate([jnp.where(m, 1.0, 0.0).astype(BF) for m in hits], axis=0)
        pre = dot(stack, up_ref[...])
        tot = jnp.concatenate([pre[rows * e:rows * e + rows, LANES:].astype(BF) for e in range(experts)], axis=1)
        before = dot(low_ref[...], tot).astype(I32)
        comb = jnp.zeros((rows, LANES), I32)
        tbl = jnp.zeros((rows, LANES), I32)
        cnt = jnp.zeros((rows, LANES), I32)
        lb = jnp.zeros((rows, LANES), I32)
        boff = lb
        for e in range(experts):
            if e % PER_CHIP == 0:
                boff = jnp.zeros((rows, LANES), I32)
            part = before[:, LANES * e:LANES * e + LANES]
            rank = pre[rows * e:rows * e + rows, :LANES].astype(I32) + part[:rows]
            s0, s1, c0, c1 = (jnp.minimum(part[rows * k:rows * k + rows], cap) for k in (1, 2, 3, 4))
            nbk = (c1 - c0 + BLK - 1) // BLK
            ss, se = s0 - c0, s1 - c0
            bs = ss // BLK
            nbl = jnp.where(se > ss, (se - 1) // BLK - bs + 1, 0)
            local = (lb - bs) * BLK + rank - c0
            comb = jnp.where(hits[e], jnp.where(rank < cap, (local + 1) * experts + e, e), comb)
            i = lane - lb
            b = boff + bs + i
            code = (2 * (e // PER_CHIP) + (b & 1)) * 4096 + (b >> 1)
            tbl = jnp.where((i >= 0) & (i < nbl), code, tbl)
            cnt = jnp.where(lane == e, nbk, cnt)
            lb = lb + nbl
            boff = boff + nbk
        tbl_ref[l] = jnp.where(lane == LANES - 1, lb, tbl)
        cnt_ref[l] = cnt
        for s in range(seqs):
            comb_ref[l, s] = comb[per_seq * s:per_seq * s + per_seq]


def route(expert_idx, cap, experts):
    layers, seqs, seq = expert_idx.shape
    rows = seqs * seq // LANES
    per_seq = seq // LANES
    r = np.arange(rows)
    edge = np.cumsum((0,) + CHUNKS) * per_seq
    which = np.searchsorted(edge, r, side='right') - 1
    starts = [r, r // per_seq * per_seq, r // per_seq * per_seq + per_seq, edge[which], edge[which + 1]]
    low = np.concatenate([(r[None, :] < s[:, None]) for s in starts]).astype(np.float32)
    k = np.arange(LANES)
    up = np.concatenate([k[:, None] < k[None, :], np.ones((LANES, LANES), bool)], axis=1).astype(np.float32)
    return pl.pallas_call(
        functools.partial(route_kernel, cap=cap, experts=experts),
        out_shape=(
            jax.ShapeDtypeStruct((layers, seqs, per_seq, LANES), I32),
            jax.ShapeDtypeStruct((layers, rows, LANES), I32),
            jax.ShapeDtypeStruct((layers, rows, LANES), I32),
        ),
        name="route",
    )(expert_idx.reshape(layers, rows, LANES), jnp.asarray(low, BF), jnp.asarray(up, BF))


def as_row(block):
    return jnp.concatenate([block[i:i + 1] for i in range(block.shape[0])], axis=1)


def as_column(row):
    return jnp.broadcast_to(row, (LANES, row.shape[1])).T


def attend(h, mask_row, gain, wq, wk, wv, wo, bias, qz, ks, vz, ctx):
    a = rms(h.astype(F32), gain).astype(BF)
    low = lax.broadcasted_iota(I32, (1, LANES), 1) < LANES // 2
    pairs = h.shape[1] // LANES
    qall = dot(a, wq[...]).astype(BF)
    kall = dot(a, wk[...]).astype(BF)
    vall = dot(a, wv[...]).astype(BF)
    zero = jnp.zeros((), BF)
    for p in range(pairs):
        sl = slice(LANES * p, LANES * p + LANES)
        q, v = qall[:, sl], vall[:, sl]
        qz[2 * p] = jnp.where(low, q, zero)
        qz[2 * p + 1] = jnp.where(low, zero, q)
        vz[2 * p] = jnp.where(low, v, zero)
        vz[2 * p + 1] = jnp.where(low, zero, v)
        ks[p] = kall[:, sl]
    neg = jnp.where(mask_row > 0, 0.0, NEG_BIG)

    def pair_body(p, carry):
        kp = ks[p]
        acc = None
        for j in range(2):
            head = 2 * p + j
            s = dot_nt(qz[head], kp) + bias[head] + neg
            m = jnp.max(s, axis=-1, keepdims=True)
            e = jnp.exp(s - m)
            z = jnp.sum(e, axis=-1, keepdims=True)
            o = dot(e.astype(BF), vz[head]) * (1.0 / z)
            acc = o if acc is None else acc + o
        ctx[p] = acc.astype(BF)
        return carry

    lax.fori_loop(0, pairs, pair_body, 0)
    c = jnp.concatenate([ctx[p] for p in range(pairs)], axis=1)
    return (h.astype(F32) + dot(c, wo[...])).astype(BF)


def gated(h1, gain, w3, comb_row, experts, rows_ref):
    h32 = h1.astype(F32)
    r = rms(h32, gain)
    hi = r.astype(BF)
    rest = r - hi.astype(F32)
    mid = rest.astype(BF)
    lo = (rest - mid.astype(F32)).astype(BF)
    part = dot(hi, w3[...]) + dot(mid, w3[...]) + dot(lo, w3[...])
    logits = part + pltpu.roll(part, LANES - experts, 1) + pltpu.roll(part, LANES - 2 * experts, 1)
    lane = lax.broadcasted_iota(I32, (1, LANES), 1)
    logits = jnp.where(lane < experts, logits, -jnp.inf)
    ex = jnp.exp(logits - jnp.max(logits, axis=-1, keepdims=True))
    col = as_column(comb_row)
    own = col & (experts - 1)
    gate = jnp.sum(jnp.where(lane == own, ex, 0.0), axis=-1, keepdims=True) / jnp.sum(ex, axis=-1, keepdims=True)
    local = (col // experts) - 1
    pick = jnp.concatenate(
        [jnp.where(lane + LANES * t == local, 1.0, 0.0).astype(BF) for t in range(LOCAL * BLK // LANES)], axis=1)
    u = dot(pick, rows_ref[...])
    return (h32 + gate * u).astype(BF)


def fetch(tbl, l, row, half, ret, rows, sem, slot, wait):
    count = tbl[l, row, LANES - 1]

    def body(i, carry):
        code = tbl[l, row, i]
        src = ((code >> 12) * half + (code & 4095)) * BLK
        copy = pltpu.make_async_copy(ret.at[pl.ds(pl.multiple_of(src, BLK), BLK)],
                                     rows.at[slot, pl.ds(pl.multiple_of(i * BLK, BLK), BLK)], sem.at[slot])
        copy.wait() if wait else copy.start()
        return carry

    lax.fori_loop(0, count, body, 0)


def returned(tbl, l, first, per_seq, half, ret, rows, sem):
    i, n = pl.program_id(0), pl.num_programs(0)
    slot = lax.rem(i, 2)

    @pl.when(i == 0)
    def _():
        rows[...] = jnp.zeros_like(rows)
        fetch(tbl, l, first * per_seq, half, ret, rows, sem, 0, False)

    fetch(tbl, l, (first + i) * per_seq, half, ret, rows, sem, slot, True)

    @pl.when(i + 1 < n)
    def _():
        fetch(tbl, l, (first + i + 1) * per_seq, half, ret, rows, sem, 1 - slot, False)

    return rows.at[slot]


def mix_kernel(tbl, h_ref, mask_ref, comb_ref, g_ref, wq, wk, wv, wo, bias, *rest,
               l, first, half, experts):
    if l:
        ret, w3, prev, h1_ref, send_ref, *rest = rest
    else:
        h1_ref, send_ref, *rest = rest
    qz, ks, vz, ctx, packed, send, sem, *rest = rest
    i, n = pl.program_id(0), pl.num_programs(0)
    per_seq = comb_ref.shape[2]
    h = h_ref[0]
    if l:
        rows, rsem = rest
        ref = returned(tbl, l - 1, first, per_seq, half, ret, rows, rsem)
        h = gated(h, g_ref[2 * l - 1:2 * l], w3, as_row(prev[0, 0]), experts, ref)

    h1 = attend(h, as_row(mask_ref[0]), g_ref[2 * l:2 * l + 1], wq, wk, wv, wo, bias, qz, ks, vz, ctx)
    h1_ref[0] = h1
    b = rms(h1.astype(F32), g_ref[2 * l + 1:2 * l + 2]).astype(BF)

    local = as_row(comb_ref[0, 0]) // experts - 1
    step = 256
    for t in range(LOCAL * BLK // step):
        at = lax.broadcasted_iota(I32, (step, 1), 0) + step * t
        pick = jnp.where(at == local, 1.0, 0.0).astype(BF)
        packed[step * t:step * t + step] = dot(pick, b).astype(BF)

    @pl.when(i == 0)
    def _():
        def clear(k, carry):
            send[pl.ds(pl.multiple_of(k * BLK, BLK), BLK)] = jnp.zeros((BLK, send.shape[1]), BF)
            return carry
        lax.fori_loop(0, send.shape[0] // BLK, clear, 0)

    row = (first + i) * per_seq

    def place(k, carry):
        code = tbl[l, row, k]
        dst = ((code >> 12) * half + (code & 4095)) * BLK
        at = pl.ds(pl.multiple_of(dst, BLK), BLK)
        send[at] = send[at] + packed[pl.ds(pl.multiple_of(k * BLK, BLK), BLK)]
        return carry

    lax.fori_loop(0, tbl[l, row, LANES - 1], place, 0)

    @pl.when(i == n - 1)
    def _():
        copy = pltpu.make_async_copy(send, send_ref, sem)
        copy.start()
        copy.wait()


def whole(a):
    return pl.BlockSpec(a.shape, lambda i, *_: (0,) * a.ndim, pipeline_mode=pl.Buffered(1))


def mix(l, first, count, half, experts, devices, tbl, h, h_first, mask, comb, gains, wq, wk, wv, wo, bias, ret=None, w3=None):
    _, seq, dim = h.shape
    heads = bias.shape[0]
    per_seq = seq // LANES
    layer = lambda a: pl.BlockSpec((None,) + a.shape[1:], lambda i, *_: (l,) + (0,) * (a.ndim - 1), pipeline_mode=pl.Buffered(1))
    any_spec = pl.BlockSpec(memory_space=pl.ANY)
    in_specs = [
        pl.BlockSpec((1, seq, dim), lambda i, *_: (h_first + i, 0, 0)),
        pl.BlockSpec((1, per_seq, LANES), lambda i, *_: (first + i, 0, 0)),
        pl.BlockSpec((1, 1, per_seq, LANES), lambda i, *_: (l, first + i, 0, 0)),
        whole(gains), layer(wq), layer(wk), layer(wv), layer(wo), whole(bias),
    ]
    args = [h, mask, comb, gains, wq, wk, wv, wo, bias]
    scratch = [
        pltpu.VMEM((heads, seq, LANES), BF), pltpu.VMEM((heads // 2, seq, LANES), BF),
        pltpu.VMEM((heads, seq, LANES), BF), pltpu.VMEM((heads // 2, seq, LANES), BF),
        pltpu.VMEM((LOCAL * BLK, dim), BF), pltpu.VMEM((devices * half * BLK, dim), BF), pltpu.SemaphoreType.DMA,
    ]
    if l:
        in_specs += [any_spec, pl.BlockSpec((None,) + w3.shape[1:], lambda i, *_: (l - 1, 0, 0), pipeline_mode=pl.Buffered(1)),
                     pl.BlockSpec((1, 1, per_seq, LANES), lambda i, *_: (l - 1, first + i, 0, 0))]
        args += [ret, w3, comb]
        scratch += [pltpu.VMEM((2, LOCAL * BLK, dim), BF), pltpu.SemaphoreType.DMA((2,))]
    flops = count * (8 * seq * dim * dim + 4 * seq * seq * dim * 4)
    return pl.pallas_call(
        functools.partial(mix_kernel, l=l, first=first, half=half, experts=experts),
        grid_spec=pltpu.PrefetchScalarGridSpec(
            num_scalar_prefetch=1, grid=(count,), in_specs=in_specs,
            out_specs=[pl.BlockSpec((1, seq, dim), lambda i, *_: (i, 0, 0)), any_spec],
            scratch_shapes=scratch),
        out_shape=[jax.ShapeDtypeStruct((count, seq, dim), BF), jax.ShapeDtypeStruct((devices * half * BLK, dim), BF)],
        compiler_params=pltpu.CompilerParams(vmem_limit_bytes=VMEM),
        cost_estimate=pl.CostEstimate(flops=flops, bytes_accessed=40 << 20, transcendentals=0),
        name=f"mix{l}",
    )(tbl, *args)


def final_kernel(tbl, h_ref, comb_ref, g_ref, w3, ret, *rest, l, first, half, experts):
    o_ref, rows, rsem = rest[-3:]
    ref = returned(tbl, l, first, comb_ref.shape[2], half, ret, rows, rsem)
    o_ref[0] = gated(h_ref[0], g_ref[2 * l + 1:2 * l + 2], w3, as_row(comb_ref[0, 0]), experts, ref)


def final(l, first, half, experts, total, tbl, h1, comb, gains, w3, ret, out=None):
    count, seq, dim = h1.shape
    per_seq = seq // LANES
    any_spec = pl.BlockSpec(memory_space=pl.ANY)
    in_specs = [
        pl.BlockSpec((1, seq, dim), lambda i, *_: (i, 0, 0)),
        pl.BlockSpec((1, 1, per_seq, LANES), lambda i, *_: (l, first + i, 0, 0)),
        whole(gains),
        pl.BlockSpec((None,) + w3.shape[1:], lambda i, *_: (l, 0, 0), pipeline_mode=pl.Buffered(1)),
        any_spec,
    ]
    args = [h1, comb, gains, w3, ret]
    if out is not None:
        in_specs.append(any_spec)
        args.append(out)
    return pl.pallas_call(
        functools.partial(final_kernel, l=l, first=first, half=half, experts=experts),
        grid_spec=pltpu.PrefetchScalarGridSpec(
            num_scalar_prefetch=1, grid=(count,), in_specs=in_specs,
            out_specs=pl.BlockSpec((1, seq, dim), lambda i, *_: (first + i, 0, 0)),
            scratch_shapes=[pltpu.VMEM((2, LOCAL * BLK, dim), BF), pltpu.SemaphoreType.DMA((2,))]),
        out_shape=jax.ShapeDtypeStruct((total, seq, dim), BF),
        input_output_aliases={} if out is None else {6: 0},
        compiler_params=pltpu.CompilerParams(vmem_limit_bytes=VMEM),
        cost_estimate=pl.CostEstimate(flops=count * 2 * seq * dim * 1024, bytes_accessed=count << 22, transcendentals=0),
        name="final",
    )(tbl, *args)


def ffn_kernel(nb, core_ref, recv, wi_own, wo_own, wi_other, wo_other, out,
               wi, wout, xb, ob, tbl, first_tile, tile_at, tile_n, wsem, isem, osem, *, l, c, half, sources):
    core = core_ref[0]

    def weights(j, wait):
        slot = lax.rem(j, 2)
        for own, (a, b) in ((True, (wi_own, wo_own)), (False, (wi_other, wo_other))):
            @pl.when((j // 2 == core) == own)
            def _():
                for src, dst, k in ((a, wi, 0), (b, wout, 1)):
                    copy = pltpu.make_async_copy(src.at[l, lax.rem(j, 2)], dst.at[slot], wsem.at[slot, k])
                    copy.wait() if wait else copy.start()

    weights(jnp.int32(0), False)

    pos = jnp.int32(0)
    tiles = jnp.int32(0)
    offs = [jnp.int32(0)] * sources
    for j in range(PER_CHIP):
        begin = pos
        for s in range(sources):
            n = nb[l, c, s * PER_CHIP + j]
            lo = (offs[s] + 1 - core) >> 1
            hi = (offs[s] + n + 1 - core) >> 1
            offs[s] = offs[s] + n
            shift = pos - lo

            def put(k, carry):
                tbl[shift + k] = s * half + k
                return carry

            lax.fori_loop(lo, hi, put, 0)
            pos = pos + hi - lo
        count = pos - begin
        nt = (count + TILE - 1) // TILE
        first_tile[j] = tiles
        base = tiles

        def mark(t, carry):
            tile_at[base + t] = begin + t * TILE
            tile_n[base + t] = jnp.minimum(TILE, count - t * TILE)
            return carry

        lax.fori_loop(0, nt, mark, 0)
        tiles = tiles + nt
    first_tile[PER_CHIP] = tiles

    def rows_in(g, wait):
        slot = lax.rem(g, 2)
        at = tile_at[g]

        def body(k, carry):
            src = tbl[at + k] * BLK
            copy = pltpu.make_async_copy(recv.at[pl.ds(pl.multiple_of(src, BLK), BLK)],
                                         xb.at[slot, pl.ds(pl.multiple_of(k * BLK, BLK), BLK)], isem.at[slot])
            copy.wait() if wait else copy.start()
            return carry

        lax.fori_loop(0, tile_n[g], body, 0)

    def rows_out(g, wait):
        slot = lax.rem(g, 2)
        at = tile_at[g]

        def body(k, carry):
            dst = tbl[at + k] * BLK
            copy = pltpu.make_async_copy(ob.at[slot, pl.ds(pl.multiple_of(k * BLK, BLK), BLK)],
                                         out.at[pl.ds(pl.multiple_of(dst, BLK), BLK)], osem.at[slot])
            copy.wait() if wait else copy.start()
            return carry

        lax.fori_loop(0, tile_n[g], body, 0)

    @pl.when(tiles > 0)
    def _():
        rows_in(jnp.int32(0), False)

    def expert(j, carry):
        weights(j, True)

        @pl.when(j + 1 < PER_CHIP)
        def _():
            weights(j + 1, False)

        ws = lax.rem(j, 2)

        def tile(g, inner):
            slot = lax.rem(g, 2)
            rows_in(g, True)

            @pl.when(g + 1 < tiles)
            def _():
                rows_in(g + 1, False)

            act = jnp.maximum(dot(xb[slot], wi[ws]), 0.0).astype(BF)
            res = dot(act, wout[ws]).astype(BF)

            @pl.when(g >= 2)
            def _():
                rows_out(g - 2, True)

            ob[slot] = res
            rows_out(g, False)
            return inner

        lax.fori_loop(first_tile[j], first_tile[j + 1], tile, 0)
        return carry

    lax.fori_loop(0, PER_CHIP, expert, 0)

    @pl.when(tiles >= 2)
    def _():
        rows_out(tiles - 2, True)

    @pl.when(tiles >= 1)
    def _():
        rows_out(tiles - 1, True)


def ffn(l, c, half, sources, nb, core, recv, wi_own, wo_own, wi_other, wo_other):
    dim, ff = wi_own.shape[2:]
    any_spec = pl.BlockSpec(memory_space=pl.ANY)
    rows = TILE * BLK
    most = sources * half + TILE * (PER_CHIP + 2)
    tiles = most // TILE + PER_CHIP + 2
    return pl.pallas_call(
        functools.partial(ffn_kernel, l=l, c=c, half=half, sources=sources),
        grid_spec=pltpu.PrefetchScalarGridSpec(
            num_scalar_prefetch=2, grid=(), in_specs=[any_spec] * 5, out_specs=any_spec,
            scratch_shapes=[
                pltpu.VMEM((2, dim, ff), BF), pltpu.VMEM((2, ff, dim), BF),
                pltpu.VMEM((2, rows, dim), BF), pltpu.VMEM((2, rows, dim), BF),
                pltpu.SMEM((most,), I32), pltpu.SMEM((PER_CHIP + 1,), I32),
                pltpu.SMEM((tiles,), I32), pltpu.SMEM((tiles,), I32),
                pltpu.SemaphoreType.DMA((2, 2)), pltpu.SemaphoreType.DMA((2,)), pltpu.SemaphoreType.DMA((2,)),
            ]),
        out_shape=jax.ShapeDtypeStruct(recv.shape, BF),
        compiler_params=pltpu.CompilerParams(vmem_limit_bytes=VMEM),
        cost_estimate=pl.CostEstimate(flops=4 * recv.shape[0] * dim * ff, bytes_accessed=40 << 20, transcendentals=0),
        name=f"ffn{l}",
    )(nb, core, recv, wi_own, wo_own, wi_other, wo_other)


def solution(mesh):
    token_spec = P(('dp', 'ep'))
    devices = mesh.shape['ep']

    def per_device(x_in, pad_mask, rel_bias, expert_idx, norm_scale, w_query, w_key, w_value, w_attn_out, w_router, w_in, w_out):
        seqs, seq, dim = x_in.shape
        layers, _, experts = w_router.shape
        cap = (CAP_FACTOR * seqs * seq + experts - 1) // experts
        firsts = [sum(CHUNKS[:c]) for c in range(len(CHUNKS))]
        per_seq = seq // LANES

        comb, tbl, cnt = route(expert_idx, cap, experts)
        mine = jnp.stack([cnt[:, f * per_seq, :experts] for f in firsts], axis=1)
        every = lax.all_gather(mine, 'ep')
        chips = experts // PER_CHIP
        by_chip = every.reshape(devices, layers, len(CHUNKS), chips, PER_CHIP)
        need = (jnp.max(jnp.sum(by_chip, axis=-1), axis=(0, 1, 3)) + 1) // 2
        me = lax.axis_index('ep')
        nb = lax.dynamic_index_in_dim(by_chip, me // 2, 3, keepdims=False)
        nb = jnp.transpose(nb, (1, 2, 0, 3)).reshape(layers, len(CHUNKS), devices * PER_CHIP)
        core = (me % 2).reshape(1)

        mask = pad_mask.reshape(seqs, per_seq, LANES)
        gains = norm_scale.reshape(2 * layers, dim)
        w_hi = w_router.astype(BF)
        rest = w_router - w_hi.astype(F32)
        w_mid = rest.astype(BF)
        w_lo = (rest - w_mid.astype(F32)).astype(BF)
        w3 = jnp.concatenate([w_hi, w_mid, w_lo, jnp.zeros((layers, dim, LANES - 3 * experts), BF)], axis=-1)

        most = tuple((min(n * seq // BLK + PER_CHIP, PER_CHIP * -(-cap // BLK)) + 1) // 2 for n in CHUNKS)
        levels = [tuple(min(round(t * n), m) for t, n, m in zip(TYPICAL, (k,) * len(CHUNKS), most)) for k in STEPS] + [most]

        def program(half):
            def run():
                swap = [(i, i ^ 1) for i in range(devices)]
                wi_other = lax.ppermute(w_in, 'ep', swap)
                wo_other = lax.ppermute(w_out, 'ep', swap)
                hidden = [(x_in, f) for f in firsts]
                ret = [None] * len(CHUNKS)
                for l in range(layers):
                    sent = []
                    for c, f in enumerate(firsts):
                        h, hf = hidden[c]
                        h1, send = mix(l, f, CHUNKS[c], half[c], experts, devices, tbl, h, hf, mask, comb, gains,
                                       w_query, w_key, w_value, w_attn_out, rel_bias,
                                       *((ret[c], w3) if l else ()))
                        hidden[c] = (h1, 0)
                        sent.append(lax.all_to_all(send, 'ep', 0, 0, tiled=True))
                    for c in range(len(CHUNKS)):
                        done = ffn(l, c, half[c], devices, nb, core, sent[c], w_in, w_out, wi_other, wo_other)
                        ret[c] = lax.all_to_all(done, 'ep', 0, 0, tiled=True)
                out = None
                for c, f in enumerate(firsts):
                    out = final(layers - 1, f, half[c], experts, seqs, tbl, hidden[c][0], comb, gains, w3, ret[c], out)
                return out
            return run

        level = sum(jnp.any(need > jnp.asarray(h, I32)).astype(I32) for h in levels[:-1])
        return lax.switch(level, [program(h) for h in levels])

    return jax.shard_map(per_device, mesh=mesh, in_specs=(token_spec, token_spec, P(), P(None, ('dp', 'ep')), P(), P(), P(), P(), P(), P(), P(None, 'ep'), P(None, 'ep')), out_specs=token_spec, check_vma=False)


TYPICAL = (41.4, 55.7)
STEPS = (0.84, 0.9, 0.96, 1.02, 1.08, 1.15, 1.25, 1.4, 1.7)
```
